1024 devices in a mesh: group: 16 (over y, core), dev: 64 (over z, x).
Axes of the slice: x: 8, y: 8, z: 8, core: 2. Of those that a mesh axis runs over, the one named last changes fastest.
Arguments:
- solution: float32 [16, 128, 16, 512], P('group', 'dev'), may hold values from -6 to 6
- residual: float32 [16, 128, 16, 512], P('group', 'dev'), may hold values from -6 to 6
- direction: float32 [16, 128, 16, 512], P('group', 'dev'), may hold values from -0.03 to 0.03
- geometry: bfloat16 [3, 16, 128, 16, 512], P(None, 'group', 'dev'), may hold values from 0.5 to 2
- mass: bfloat16 [16, 128, 16, 512], P('group', 'dev'), may hold values from 50 to 500
Outputs:
- solution_out: float32 [16, 128, 16, 512], P('group', 'dev')
- residual_out: float32 [16, 128, 16, 512], P('group', 'dev')
- direction_out: float32 [16, 128, 16, 512], P('group', 'dev')
The draws below stay inside these ranges and needn't reach their ends.
All inputs are finite; a program needn't handle non-finite values.
Results may differ from the reference program's by a relative error of at most 0.0003.
Values sent between devices are 32-bit elements; how exact they have to be, the bound alone decides.
No kernel may reach another device: no remote copies, remote signals or barrier semaphores. Data moves between devices by JAX's collectives and lax.ppermute only.
A program may use at most 32 MiB of HBM per device.

```python
import math
import jax
import jax.numpy as jnp
import numpy as np
from jax import lax

NP = 8
EZ = 16
EA = 16
EB = 128


def draw_direction(key, part):
    position = jnp.arange(EA, dtype=jnp.float32) / max(EA - 1, 1)
    shape = (EA, EB, EZ, NP ** 3)
    noise = jnp.clip(jax.random.normal(key, shape, jnp.float32), -6.0, 6.0)
    rise = jnp.power(4.0, position)
    return (0.001 * rise[:, None, None, None] * noise).astype(jnp.float32)


def level_of(stream_key, dims, split, least, largest):
    factor_of, own = 1.0, jax.random.fold_in(stream_key, 6)
    for dim, parts in split:
        steps = jnp.exp(jax.random.uniform(jax.random.fold_in(own, dim), (parts,), jnp.float32, least / len(split), largest / len(split)))
        factor_of = factor_of * jnp.repeat(steps, dims[dim] // parts).reshape([-1 if axis == dim else 1 for axis in range(len(dims))])
    return factor_of


def centred(key, dims, deviation, limit, shards=(), kind=jnp.bfloat16):
    entries = deviation * jax.random.normal(key, dims, jnp.float32)
    if shards:
        entries = entries * level_of(key, dims, shards, -0.22, 0.18)
    return jnp.clip(entries, -limit, limit).astype(kind)


def setup_inputs(seed: int = 0) -> dict:
    splits = jax.random.split(jax.random.key(seed), 6)
    solution = centred(splits[0], (EA, EB, EZ, NP ** 3), 1.0, 6.0, ((0, 16), (1, 64)), jnp.float32)
    residual = centred(splits[1], (EA, EB, EZ, NP ** 3), 1.0, 6.0, ((0, 16), (1, 64)), jnp.float32)
    direction = draw_direction(jax.random.fold_in(splits[5], 71), 0)
    geometry = jnp.clip(jnp.exp(math.log(2.0) - 1.3862944 * jax.random.uniform(splits[3], (3, EA, EB, EZ, NP ** 3), jnp.float32) ** level_of(splits[3], (3, EA, EB, EZ, NP ** 3), ((1, 16), (2, 64)), -0.2, 0.2)), 0.5, 2.0).astype(jnp.bfloat16)
    mass = jnp.clip(jnp.exp(math.log(500.0) - 2.3025851 * jax.random.uniform(splits[4], (EA, EB, EZ, NP ** 3), jnp.float32) ** level_of(splits[4], (EA, EB, EZ, NP ** 3), ((0, 16), (1, 64)), -0.2, 0.2)), 50.0, 500.0).astype(jnp.bfloat16)
    return {"solution": solution, "residual": residual, "direction": direction, "geometry": geometry, "mass": mass}


lobatto_nodes = [-1.0, -0.8717401485096066, -0.5917001814331423, -0.2092992179024789,
                 0.2092992179024789, 0.5917001814331423, 0.8717401485096066, 1.0]


def derivative_table():
    nodes = np.array(lobatto_nodes)
    identity = np.eye(NP)
    offset = nodes[:, None] - nodes[None, :] + identity
    barycentric = 1.0 / np.prod(offset, axis=1)
    derivative = (barycentric[None, :] / barycentric[:, None]) / offset * (1.0 - identity)
    return derivative - identity * np.sum(derivative, axis=1)[:, None]


def operator_tables():
    derivative = derivative_table()
    identity = np.eye(NP)
    kron_list = [np.kron(np.kron(derivative, identity), identity),
                 np.kron(np.kron(identity, derivative), identity),
                 np.kron(np.kron(identity, identity), derivative)]
    forward = np.concatenate([matrix.T for matrix in kron_list], axis=1)
    backward = np.concatenate(kron_list, axis=0)
    squares = np.concatenate([matrix * matrix for matrix in kron_list], axis=0)
    return (jnp.asarray(forward, dtype=jnp.float32), jnp.asarray(backward, dtype=jnp.float32),
            jnp.asarray(squares, dtype=jnp.float32))


def point_weights():
    edge = np.where(np.arange(NP) % (NP - 1) == 0, 0.5, 1.0)
    return jnp.asarray(np.kron(np.kron(edge, edge), edge), dtype=jnp.float32)


def highest(left, right):
    return jnp.dot(left, right, precision=lax.Precision.HIGHEST, preferred_element_type=jnp.float32)


def face_pass(field, elem_dim, node_dim):
    lower = lax.index_in_dim(field, 0, node_dim, keepdims=True)
    upper = lax.index_in_dim(field, NP - 1, node_dim, keepdims=True)
    summed = upper + jnp.roll(lower, -1, axis=elem_dim)
    middle = lax.slice_in_dim(field, 1, NP - 1, axis=node_dim)
    return jnp.concatenate([jnp.roll(summed, 1, axis=elem_dim), middle, summed], axis=node_dim)


def assemble(field):
    shaped = field.reshape(field.shape[:3] + (NP, NP, NP))
    shaped = face_pass(shaped, 0, 3)
    shaped = face_pass(shaped, 1, 4)
    shaped = face_pass(shaped, 2, 5)
    return shaped.reshape(field.shape)


def reference(solution, residual, direction, geometry, mass):
    forward, backward, squares = operator_tables()
    weights = point_weights()
    points = NP ** 3
    geometry_rows = jnp.moveaxis(geometry.astype(jnp.float32), 0, -2)
    geometry_rows = geometry_rows.reshape(solution.shape[:3] + (3 * points,))
    mass_coef = mass.astype(jnp.float32)

    def diagonal_block(pair):
        geo_block, mass_block = pair
        flat = geo_block.reshape(-1, 3 * points)
        return (highest(flat, squares).reshape(mass_block.shape) + mass_block)

    def operator_block(triple):
        field_block, geo_block, mass_block = triple
        flat = field_block.reshape(-1, points)
        gradients = highest(flat, forward)
        fluxes = geo_block.reshape(-1, 3 * points) * gradients
        result = highest(fluxes, backward) + mass_block.reshape(-1, points) * flat
        return result.reshape(field_block.shape)

    diagonal = assemble(lax.map(diagonal_block, (geometry_rows, mass_coef)))
    smooth = assemble(weights * direction)
    scaled = residual / diagonal
    norm_now = jnp.sum(weights * residual * scaled)
    applied = assemble(lax.map(operator_block, (smooth, geometry_rows, mass_coef)))
    curvature = jnp.sum(weights * smooth * applied)
    step_size = norm_now / curvature
    solution_out = solution + step_size * smooth
    residual_out = residual - step_size * applied
    norm_next = jnp.sum(weights * residual_out * residual_out / diagonal)
    direction_out = residual_out / diagonal + (norm_next / norm_now) * smooth
    return (solution_out, residual_out, direction_out)
```

```python
import jax
import jax.numpy as jnp
import numpy as np
from jax import lax
from jax.experimental import pallas as pl
from jax.experimental.pallas import tpu as pltpu
from jax.sharding import PartitionSpec as P

NP = 8
LANES = 128
TILES = NP**3 // LANES
HALF = NP * NP

lobatto_nodes = [
    -1.0,
    -0.8717401485096066,
    -0.5917001814331423,
    -0.2092992179024789,
    0.2092992179024789,
    0.5917001814331423,
    0.8717401485096066,
    1.0,
]


def derivative_table():
    nodes = np.array(lobatto_nodes)
    identity = np.eye(NP)
    offset = nodes[:, None] - nodes[None, :] + identity
    barycentric = 1.0 / np.prod(offset, axis=1)
    derivative = barycentric[None, :] / barycentric[:, None] / offset * (1.0 - identity)
    return derivative - identity * np.sum(derivative, axis=1)[:, None]


def lane_tables():
    derivative = derivative_table()
    half = np.arange(LANES) // HALF
    rows = []
    for matrix in (derivative, derivative.T):
        for out in range(TILES):
            for inp in range(TILES):
                rows.append(matrix[2 * out + half, 2 * inp + half])
                rows.append(matrix[2 * out + half, 2 * inp + 1 - half])
    edge = np.where(np.arange(NP) % (NP - 1) == 0, 0.5, 1.0)
    rows.extend(np.kron(np.kron(edge, edge), edge).reshape(TILES, LANES))
    rows.extend(np.zeros((72 - len(rows), LANES)))
    return np.stack(rows).astype(np.float32)


def plane_table():
    derivative = derivative_table()
    identity = np.eye(NP)
    along_j = np.kron(np.eye(2), np.kron(derivative, identity))
    along_k = np.kron(np.eye(2), np.kron(identity, derivative))
    return np.concatenate([along_j.T, along_k.T], axis=1).astype(np.float32)


def lanes(rows):
    return lax.broadcasted_iota(jnp.int32, (rows, LANES), 1)


def roll(value, shift, axis):
    return pltpu.roll(value, shift % value.shape[axis], axis)


def split(value, dims):
    eb, ez = dims
    return [
        [value[b * ez : (b + 1) * ez, t * LANES : (t + 1) * LANES] for b in range(eb)]
        for t in range(TILES)
    ]


def join(blocks):
    return jnp.concatenate([jnp.concatenate(tile, axis=0) for tile in blocks], axis=1)


def local_assemble(blocks):
    result = []
    for tile in blocks:
        lane = lanes(tile[0].shape[0])
        k = lane % NP
        j = (lane // NP) % NP
        summed = []
        for x in tile:
            above = roll(roll(x, NP - 1, 1), -1, 0)
            below = roll(roll(x, 1 - NP, 1), 1, 0)
            summed.append(x + jnp.where(k == NP - 1, above, jnp.where(k == 0, below, 0.0)))
        out = []
        last = len(summed) - 1
        for b, x in enumerate(summed):
            y = x
            if b < last:
                y = y + jnp.where(j == NP - 1, roll(summed[b + 1], HALF - NP, 1), 0.0)
            if b > 0:
                y = y + jnp.where(j == 0, roll(summed[b - 1], NP - HALF, 1), 0.0)
            out.append(y)
        result.append(out)
    return result


def pack_dev(fields, block, node):
    rows = fields[0][0][block].shape[0]
    lane = lanes(rows)
    packed = jnp.zeros((rows, LANES), jnp.float32)
    for f, blocks in enumerate(fields):
        for i in range(NP):
            t, h = divmod(i, 2)
            target = f * HALF + i * NP
            source = h * HALF + node * NP
            moved = roll(blocks[t][block], target - source, 1)
            packed = jnp.where(lane // NP == target // NP, moved, packed)
    return packed


def unpack_dev(packed, field, node, tile):
    lane = lanes(packed.shape[0])
    result = jnp.zeros(packed.shape, jnp.float32)
    for h in range(2):
        source = field * HALF + (2 * tile + h) * NP
        target = h * HALF + node * NP
        result = jnp.where(lane // NP == target // NP, roll(packed, target - source, 1), result)
    return result


def pack_group(fields, upper):
    tile = TILES - 1 if upper else 0
    parts = [jnp.concatenate(blocks[tile], axis=0) for blocks in fields]
    lane = lanes(parts[0].shape[0])
    if upper:
        parts[0] = roll(parts[0], HALF, 1)
    else:
        parts[1:] = [roll(part, HALF, 1) for part in parts[1:]]
    other = parts[1] if len(parts) > 1 else 0.0
    return jnp.where(lane < HALF, parts[0], other)


def add_dev(blocks, field, before, after):
    out = []
    for t, tile in enumerate(blocks):
        tile = list(tile)
        tile[0] = tile[0] + unpack_dev(before, field, 0, t)
        tile[-1] = tile[-1] + unpack_dev(after, field, NP - 1, t)
        out.append(tile)
    return out


def add_group(blocks, field, before, after):
    eb = len(blocks[0])
    ez = blocks[0][0].shape[0]
    lane = lanes(ez)
    out = [list(tile) for tile in blocks]
    for b in range(eb):
        low = before[b * ez : (b + 1) * ez, :]
        high = after[b * ez : (b + 1) * ez, :]
        if field:
            low = roll(low, HALF, 1)
        else:
            high = roll(high, HALF, 1)
        out[0][b] = out[0][b] + jnp.where(lane < HALF, low, 0.0)
        out[-1][b] = out[-1][b] + jnp.where(lane >= HALF, high, 0.0)
    return out


def first_direction(tables, base, tiles, squared=False):
    swapped = [roll(tile, HALF, 1) for tile in tiles]
    out = []
    for o in range(TILES):
        acc = None
        for i in range(TILES):
            row = base + 2 * (o * TILES + i)
            same = tables[row : row + 1, :]
            other = tables[row + 1 : row + 2, :]
            if squared:
                same, other = same * same, other * other
            term = same * tiles[i] + other * swapped[i]
            acc = term if acc is None else acc + term
        out.append(acc)
    return out


def matmul(left, right):
    return lax.dot_general(
        left,
        right,
        (((1,), (0,)), ((), ())),
        precision=lax.Precision.HIGHEST,
        preferred_element_type=jnp.float32,
    )


def matmul_t(left, right):
    return lax.dot_general(
        left,
        right,
        (((1,), (1,)), ((), ())),
        precision=lax.Precision.HIGHEST,
        preferred_element_type=jnp.float32,
    )


def tiles_of(value):
    return [value[:, t * LANES : (t + 1) * LANES] for t in range(TILES)]


def stack_rows(tiles):
    return jnp.concatenate(tiles, axis=0)


def unstack_rows(value):
    rows = value.shape[0] // TILES
    return [value[t * rows : (t + 1) * rows, :] for t in range(TILES)]


def blocks_of(tiles, dims):
    eb, ez = dims
    return [[tile[b * ez : (b + 1) * ez, :] for b in range(eb)] for tile in tiles]


def start_kernel(dims, direction, tables, field_out, dev_low, dev_high, group_low, group_high):
    weighted = [
        tables[64 + t : 65 + t, :] * direction[:, t * LANES : (t + 1) * LANES] for t in range(TILES)
    ]
    blocks = local_assemble(blocks_of(weighted, dims))
    field_out[...] = join(blocks)
    dev_low[...] = pack_dev([blocks], 0, 0)
    dev_high[...] = pack_dev([blocks], dims[0] - 1, NP - 1)
    group_low[...] = pack_group([blocks], False)
    group_high[...] = pack_group([blocks], True)


def diagonal_kernel(dims, geometry, mass, plane, tables, diag_out):
    geo = [tiles_of(geometry[c].astype(jnp.float32)) for c in range(3)]
    first = first_direction(tables, 32, geo[0], squared=True)
    table = plane[...]
    pair = jnp.concatenate([stack_rows(geo[1]), stack_rows(geo[2])], axis=1)
    rest = unstack_rows(matmul_t(pair, table * table))
    masses = tiles_of(mass[...].astype(jnp.float32))
    local = [a + b + c for a, b, c in zip(first, rest, masses)]
    diag_out[...] = join(local_assemble(blocks_of(local, dims)))


def corner_kernel(dims, group_low, group_high, before, after, low_out, high_out):
    eb, ez = dims
    low_recv = before[...]
    high_recv = after[...]
    lane = lanes(ez)
    j = (lane // NP) % NP
    for ref, out, upper in ((group_low, low_out, False), (group_high, high_out, True)):
        shift_low = NP - HALF if upper else 0
        shift_high = 0 if upper else HALF - NP
        blocks = [ref[b * ez : (b + 1) * ez, :] for b in range(eb)]
        low = roll(low_recv, shift_low, 1) if shift_low else low_recv
        high = roll(high_recv, shift_high, 1) if shift_high else high_recv
        blocks[0] = blocks[0] + jnp.where(j == 0, low, 0.0)
        blocks[-1] = blocks[-1] + jnp.where(j == NP - 1, high, 0.0)
        for b in range(eb):
            out[b * ez : (b + 1) * ez, :] = blocks[b]


def operator_kernel(
    dims,
    field,
    dev_before,
    dev_after,
    group_before,
    group_after,
    geometry,
    mass,
    plane,
    tables,
    diag,
    smooth_out,
    applied_out,
    dev_low,
    dev_high,
    group_low,
    group_high,
):
    blocks = split(field, dims)
    blocks = add_dev(blocks, 0, dev_before[...], dev_after[...])
    blocks = add_group(blocks, 0, group_before, group_after)
    smooth_out[...] = join(blocks)
    tiles = [jnp.concatenate(tile, axis=0) for tile in blocks]
    geo = [tiles_of(geometry[c].astype(jnp.float32)) for c in range(3)]
    table = plane[...]
    first = [g * f for g, f in zip(geo[0], first_direction(tables, 0, tiles))]
    gradient = matmul(stack_rows(tiles), table)
    pair = jnp.concatenate([stack_rows(geo[1]), stack_rows(geo[2])], axis=1) * gradient
    rest = unstack_rows(matmul_t(pair, table))
    first = first_direction(tables, 32, first)
    masses = tiles_of(mass[...].astype(jnp.float32))
    local = [a + b + m * u for a, b, m, u in zip(first, rest, masses, tiles)]
    blocks = local_assemble(blocks_of(local, dims))
    applied_out[...] = join(blocks)
    diag_blocks = split(diag, dims)
    dev_low[...] = pack_dev([blocks, diag_blocks], 0, 0)
    dev_high[...] = pack_dev([blocks, diag_blocks], dims[0] - 1, NP - 1)
    group_low[...] = pack_group([blocks, diag_blocks], False)
    group_high[...] = pack_group([blocks, diag_blocks], True)


def products_kernel(
    dims,
    field,
    diag,
    dev_before,
    dev_after,
    group_before,
    group_after,
    residual,
    smooth,
    tables,
    applied_out,
    inverse_out,
    sums_out,
):
    full = []
    for index, ref in enumerate((field, diag)):
        blocks = add_dev(split(ref, dims), index, dev_before[...], dev_after[...])
        blocks = add_group(blocks, index, group_before, group_after)
        full.append([jnp.concatenate(tile, axis=0) for tile in blocks])
    sums = [None] * 4
    for t in range(TILES):
        window = slice(t * LANES, (t + 1) * LANES)
        weight = tables[64 + t : 65 + t, :]
        applied = full[0][t]
        inverse = 1.0 / full[1][t]
        applied_out[:, window] = applied
        inverse_out[:, window] = inverse
        res = residual[:, window]
        weighted = weight * inverse
        terms = (
            weighted * res * res,
            weight * smooth[:, window] * applied,
            weighted * res * applied,
            weighted * applied * applied,
        )
        sums = [term if s is None else s + term for s, term in zip(sums, terms)]
    lane = lanes(1)
    row = jnp.zeros((1, LANES), jnp.float32)
    for n, total in enumerate(sums):
        column = jnp.sum(total, axis=0, keepdims=True)
        row = jnp.where(lane == n, jnp.sum(column, axis=1, keepdims=True), row)
    sums_out[...] = jnp.broadcast_to(row.reshape(1, 1, LANES), sums_out.shape)


def middle_kernel(parts, sums_out):
    total = jnp.sum(parts[...], axis=0, keepdims=True)
    sums_out[...] = jnp.broadcast_to(total, sums_out.shape)


def final_kernel(
    parts, solution, residual, smooth, applied, inverse, solution_out, residual_out, direction_out
):
    total = jnp.sum(parts[...], axis=0)
    norm_now, curvature, cross, quad = (total[:, n : n + 1] for n in range(4))
    step = norm_now / curvature
    norm_next = norm_now - 2.0 * step * cross + step * step * quad
    ratio = norm_next / norm_now
    direction = smooth[...]
    res = residual[...] - step * applied[...]
    solution_out[...] = solution[...] + step * direction
    residual_out[...] = res
    direction_out[...] = res * inverse[...] + ratio * direction


def call(kernel, shapes, *args):
    outs = tuple(jax.ShapeDtypeStruct(shape, jnp.float32) for shape in shapes)
    vmem = pl.BlockSpec(memory_space=pltpu.VMEM)
    return pl.pallas_call(
        kernel,
        out_shape=outs,
        in_specs=[vmem] * len(args),
        out_specs=(vmem,) * len(outs),
        compiler_params=pltpu.CompilerParams(vmem_limit_bytes=8 * 2**20),
    )(*args)


def both_ways(low, high, axis):
    peers = lax.axis_size(axis)
    up = [(i, (i + 1) % peers) for i in range(peers)]
    before = lax.ppermute(high, axis, up)
    after = lax.ppermute(low, axis, [(j, i) for i, j in up])
    return before, after


def solution(mesh):
    groups = mesh.shape["group"]
    devs = mesh.shape["dev"]

    def on_device(solution, residual, direction, geometry, mass):
        local = solution.shape
        dims = local[1:3]
        rows = dims[0] * dims[1]
        points = local[3]
        flat = (rows, points)
        face_dev = (dims[1], LANES)
        face_group = (rows, LANES)
        solution, residual, direction, mass = (
            array.reshape(flat) for array in (solution, residual, direction, mass)
        )
        geometry = geometry.reshape((3,) + flat)
        tables = jnp.asarray(lane_tables())
        plane = jnp.asarray(plane_table())

        def bind(kernel):
            def body(*refs):
                kernel(dims, *refs)

            body.__name__ = kernel.__name__
            return body

        corners = bind(corner_kernel)
        field, dev_low, dev_high, group_low, group_high = call(
            bind(start_kernel),
            [flat, face_dev, face_dev, face_group, face_group],
            direction,
            tables,
        )
        dev = both_ways(dev_low, dev_high, "dev")
        (diag,) = call(bind(diagonal_kernel), [flat], geometry, mass, plane, tables)
        low, high = call(corners, [face_group] * 2, group_low, group_high, *dev)
        group = both_ways(low, high, "group")
        smooth, applied, dev_low, dev_high, group_low, group_high = call(
            bind(operator_kernel),
            [flat, flat, face_dev, face_dev, face_group, face_group],
            field,
            *dev,
            *group,
            geometry,
            mass,
            plane,
            tables,
            diag,
        )
        dev = both_ways(dev_low, dev_high, "dev")
        low, high = call(corners, [face_group] * 2, group_low, group_high, *dev)
        group = both_ways(low, high, "group")
        applied, inverse, sums = call(
            bind(products_kernel),
            [flat, flat, (devs, 1, LANES)],
            applied,
            diag,
            *dev,
            *group,
            residual,
            smooth,
            tables,
        )
        sums = lax.all_to_all(sums, "dev", 0, 0)
        (sums,) = call(middle_kernel, [(groups, 1, LANES)], sums)
        sums = lax.all_to_all(sums, "group", 0, 0)
        outs = call(
            final_kernel, [flat] * 3, sums, solution, residual, smooth, applied, inverse
        )
        return tuple(out.reshape(local) for out in outs)

    spec = P("group", "dev", None, None)
    return jax.shard_map(
        on_device,
        mesh=mesh,
        in_specs=(spec, spec, spec, P(None, "group", "dev", None, None), spec),
        out_specs=(spec, spec, spec),
        check_vma=False,
    )
```

```python
import jax
import jax.numpy as jnp
import numpy as np
from jax import lax
from jax.experimental import pallas as pl
from jax.experimental.pallas import tpu as pltpu
from jax.sharding import PartitionSpec as P

NP = 8
LANES = 128
TILES = NP**3 // LANES
HALF = NP * NP
SECOND = 64

lobatto_nodes = [
    -1.0,
    -0.8717401485096066,
    -0.5917001814331423,
    -0.2092992179024789,
    0.2092992179024789,
    0.5917001814331423,
    0.8717401485096066,
    1.0,
]


def derivative_table():
    nodes = np.array(lobatto_nodes)
    identity = np.eye(NP)
    offset = nodes[:, None] - nodes[None, :] + identity
    barycentric = 1.0 / np.prod(offset, axis=1)
    derivative = barycentric[None, :] / barycentric[:, None] / offset * (1.0 - identity)
    return derivative - identity * np.sum(derivative, axis=1)[:, None]


def lane_tables():
    derivative = derivative_table()
    half = np.arange(LANES) // HALF
    rows = []
    for matrix in (derivative, derivative.T):
        for out in range(TILES):
            for inp in range(TILES):
                rows.append(matrix[2 * out + half, 2 * inp + half])
                rows.append(matrix[2 * out + half, 2 * inp + 1 - half])
    lane = np.arange(LANES)
    rows.extend(derivative[(lane // NP) % NP, node] for node in range(NP))
    rows.extend(derivative[lane % NP, node] for node in range(NP))
    return np.stack(rows).astype(np.float32)


def lanes(rows):
    return lax.broadcasted_iota(jnp.int32, (rows, LANES), 1)


def plane_table(tables):
    lane = lanes(NP)
    sub = lax.broadcasted_iota(jnp.int32, (NP, LANES), 0)
    same_k = lane % NP == sub
    along_k = tables[SECOND + NP : SECOND + 2 * NP, :]
    parts_j, parts_k = [], []
    for block in range(LANES // NP):
        half, j = divmod(block, NP)
        along_j = jnp.broadcast_to(tables[SECOND + j : SECOND + j + 1, :], (NP, LANES))
        parts_j.append(jnp.where(same_k & (lane // HALF == half), along_j, 0.0))
        parts_k.append(jnp.where(lane // NP == block, along_k, 0.0))
    return jnp.concatenate(
        [jnp.concatenate(parts_j, axis=0), jnp.concatenate(parts_k, axis=0)], axis=1
    )


def lane_weights(tile):
    lane = lanes(1)
    i = 2 * tile + lane // HALF
    weight = jnp.ones((1, LANES), jnp.float32)
    for node in (i, (lane // NP) % NP, lane % NP):
        weight = weight * jnp.where((node == 0) | (node == NP - 1), 0.5, 1.0)
    return weight


def roll(value, shift, axis):
    return pltpu.roll(value, shift % value.shape[axis], axis)


def split(value, dims):
    eb, ez = dims
    return [
        [value[b * ez : (b + 1) * ez, t * LANES : (t + 1) * LANES] for b in range(eb)]
        for t in range(TILES)
    ]


def join(blocks):
    return jnp.concatenate([jnp.concatenate(tile, axis=0) for tile in blocks], axis=1)


def local_assemble(blocks):
    result = []
    for tile in blocks:
        lane = lanes(tile[0].shape[0])
        k = lane % NP
        j = (lane // NP) % NP
        summed = []
        for x in tile:
            above = roll(roll(x, NP - 1, 1), -1, 0)
            below = roll(roll(x, 1 - NP, 1), 1, 0)
            summed.append(x + jnp.where(k == NP - 1, above, jnp.where(k == 0, below, 0.0)))
        out = []
        last = len(summed) - 1
        for b, x in enumerate(summed):
            y = x
            if b < last:
                y = y + jnp.where(j == NP - 1, roll(summed[b + 1], HALF - NP, 1), 0.0)
            if b > 0:
                y = y + jnp.where(j == 0, roll(summed[b - 1], NP - HALF, 1), 0.0)
            out.append(y)
        result.append(out)
    return result


def pack_dev(fields, block, node):
    rows = fields[0][0][block].shape[0]
    lane = lanes(rows)
    packed = jnp.zeros((rows, LANES), jnp.float32)
    for f, blocks in enumerate(fields):
        for i in range(NP):
            t, h = divmod(i, 2)
            target = f * HALF + i * NP
            source = h * HALF + node * NP
            moved = roll(blocks[t][block], target - source, 1)
            packed = jnp.where(lane // NP == target // NP, moved, packed)
    return packed


def unpack_dev(packed, field, node, tile):
    lane = lanes(packed.shape[0])
    result = jnp.zeros(packed.shape, jnp.float32)
    for h in range(2):
        source = field * HALF + (2 * tile + h) * NP
        target = h * HALF + node * NP
        result = jnp.where(lane // NP == target // NP, roll(packed, target - source, 1), result)
    return result


def pack_group(fields, upper):
    tile = TILES - 1 if upper else 0
    parts = [jnp.concatenate(blocks[tile], axis=0) for blocks in fields]
    lane = lanes(parts[0].shape[0])
    if upper:
        parts[0] = roll(parts[0], HALF, 1)
    else:
        parts[1:] = [roll(part, HALF, 1) for part in parts[1:]]
    other = parts[1] if len(parts) > 1 else 0.0
    return jnp.where(lane < HALF, parts[0], other)


def add_dev(blocks, field, before, after):
    out = []
    for t, tile in enumerate(blocks):
        tile = list(tile)
        tile[0] = tile[0] + unpack_dev(before, field, 0, t)
        tile[-1] = tile[-1] + unpack_dev(after, field, NP - 1, t)
        out.append(tile)
    return out


def add_group(blocks, field, before, after):
    eb = len(blocks[0])
    ez = blocks[0][0].shape[0]
    lane = lanes(ez)
    out = [list(tile) for tile in blocks]
    for b in range(eb):
        low = before[b * ez : (b + 1) * ez, :]
        high = after[b * ez : (b + 1) * ez, :]
        if field:
            low = roll(low, HALF, 1)
        else:
            high = roll(high, HALF, 1)
        out[0][b] = out[0][b] + jnp.where(lane < HALF, low, 0.0)
        out[-1][b] = out[-1][b] + jnp.where(lane >= HALF, high, 0.0)
    return out


def first_direction(tables, base, tiles, squared=False):
    swapped = [roll(tile, HALF, 1) for tile in tiles]
    out = []
    for o in range(TILES):
        acc = None
        for i in range(TILES):
            row = base + 2 * (o * TILES + i)
            same = tables[row : row + 1, :]
            other = tables[row + 1 : row + 2, :]
            if squared:
                same, other = same * same, other * other
            term = same * tiles[i] + other * swapped[i]
            acc = term if acc is None else acc + term
        out.append(acc)
    return out


def matmul(left, right):
    return lax.dot_general(
        left,
        right,
        (((1,), (0,)), ((), ())),
        precision=lax.Precision.HIGHEST,
        preferred_element_type=jnp.float32,
    )


def matmul_t(left, right):
    return lax.dot_general(
        left,
        right,
        (((1,), (1,)), ((), ())),
        precision=lax.Precision.HIGHEST,
        preferred_element_type=jnp.float32,
    )


def tiles_of(value):
    return [value[:, t * LANES : (t + 1) * LANES] for t in range(TILES)]


def stack_rows(tiles):
    return jnp.concatenate(tiles, axis=0)


def unstack_rows(value):
    rows = value.shape[0] // TILES
    return [value[t * rows : (t + 1) * rows, :] for t in range(TILES)]


def blocks_of(tiles, dims):
    eb, ez = dims
    return [[tile[b * ez : (b + 1) * ez, :] for b in range(eb)] for tile in tiles]


def start_kernel(dims, direction, field_out, dev_low, dev_high, group_low, group_high):
    weighted = [
        lane_weights(t) * direction[:, t * LANES : (t + 1) * LANES] for t in range(TILES)
    ]
    blocks = local_assemble(blocks_of(weighted, dims))
    field_out[...] = join(blocks)
    dev_low[...] = pack_dev([blocks], 0, 0)
    dev_high[...] = pack_dev([blocks], dims[0] - 1, NP - 1)
    group_low[...] = pack_group([blocks], False)
    group_high[...] = pack_group([blocks], True)


def diagonal_kernel(dims, geometry, mass, tables, diag_out, tables_out, plane_out):
    geo = [tiles_of(geometry[c].astype(jnp.float32)) for c in range(3)]
    first = first_direction(tables, 32, geo[0], squared=True)
    table = plane_table(tables)
    tables_out[...] = tables[...]
    plane_out[...] = table
    pair = jnp.concatenate([stack_rows(geo[1]), stack_rows(geo[2])], axis=1)
    rest = unstack_rows(matmul_t(pair, table * table))
    masses = tiles_of(mass[...].astype(jnp.float32))
    local = [a + b + c for a, b, c in zip(first, rest, masses)]
    diag_out[...] = join(local_assemble(blocks_of(local, dims)))


def corner_kernel(dims, group_low, group_high, before, after, low_out, high_out):
    eb, ez = dims
    low_recv = before[...]
    high_recv = after[...]
    lane = lanes(ez)
    j = (lane // NP) % NP
    for ref, out, upper in ((group_low, low_out, False), (group_high, high_out, True)):
        shift_low = NP - HALF if upper else 0
        shift_high = 0 if upper else HALF - NP
        blocks = [ref[b * ez : (b + 1) * ez, :] for b in range(eb)]
        low = roll(low_recv, shift_low, 1) if shift_low else low_recv
        high = roll(high_recv, shift_high, 1) if shift_high else high_recv
        blocks[0] = blocks[0] + jnp.where(j == 0, low, 0.0)
        blocks[-1] = blocks[-1] + jnp.where(j == NP - 1, high, 0.0)
        for b in range(eb):
            out[b * ez : (b + 1) * ez, :] = blocks[b]


def operator_kernel(
    dims,
    field,
    dev_before,
    dev_after,
    group_before,
    group_after,
    geometry,
    mass,
    tables,
    plane,
    diag,
    smooth_out,
    applied_out,
    dev_low,
    dev_high,
    group_low,
    group_high,
):
    blocks = split(field, dims)
    blocks = add_dev(blocks, 0, dev_before[...], dev_after[...])
    blocks = add_group(blocks, 0, group_before, group_after)
    smooth_out[...] = join(blocks)
    tiles = [jnp.concatenate(tile, axis=0) for tile in blocks]
    geo = [tiles_of(geometry[c].astype(jnp.float32)) for c in range(3)]
    table = plane[...]
    first = [g * f for g, f in zip(geo[0], first_direction(tables, 0, tiles))]
    gradient = matmul(stack_rows(tiles), table)
    pair = jnp.concatenate([stack_rows(geo[1]), stack_rows(geo[2])], axis=1) * gradient
    rest = unstack_rows(matmul_t(pair, table))
    first = first_direction(tables, 32, first)
    masses = tiles_of(mass[...].astype(jnp.float32))
    local = [a + b + m * u for a, b, m, u in zip(first, rest, masses, tiles)]
    blocks = local_assemble(blocks_of(local, dims))
    applied_out[...] = join(blocks)
    diag_blocks = split(diag, dims)
    dev_low[...] = pack_dev([blocks, diag_blocks], 0, 0)
    dev_high[...] = pack_dev([blocks, diag_blocks], dims[0] - 1, NP - 1)
    group_low[...] = pack_group([blocks, diag_blocks], False)
    group_high[...] = pack_group([blocks, diag_blocks], True)


def products_kernel(
    dims,
    field,
    diag,
    dev_before,
    dev_after,
    group_before,
    group_after,
    residual,
    smooth,
    applied_out,
    inverse_out,
    sums_out,
):
    full = []
    for index, ref in enumerate((field, diag)):
        blocks = add_dev(split(ref, dims), index, dev_before[...], dev_after[...])
        blocks = add_group(blocks, index, group_before, group_after)
        full.append([jnp.concatenate(tile, axis=0) for tile in blocks])
    sums = [None] * 4
    for t in range(TILES):
        window = slice(t * LANES, (t + 1) * LANES)
        weight = lane_weights(t)
        applied = full[0][t]
        inverse = 1.0 / full[1][t]
        applied_out[:, window] = applied
        inverse_out[:, window] = inverse
        res = residual[:, window]
        weighted = weight * inverse
        terms = (
            weighted * res * res,
            weight * smooth[:, window] * applied,
            weighted * res * applied,
            weighted * applied * applied,
        )
        sums = [term if s is None else s + term for s, term in zip(sums, terms)]
    lane = lanes(1)
    row = jnp.zeros((1, LANES), jnp.float32)
    for n, total in enumerate(sums):
        column = jnp.sum(total, axis=0, keepdims=True)
        row = jnp.where(lane == n, jnp.sum(column, axis=1, keepdims=True), row)
    sums_out[...] = jnp.broadcast_to(row.reshape(1, 1, LANES), sums_out.shape)


def middle_kernel(parts, sums_out):
    total = jnp.sum(parts[...], axis=0, keepdims=True)
    sums_out[...] = jnp.broadcast_to(total, sums_out.shape)


def final_kernel(
    parts, solution, residual, smooth, applied, inverse, solution_out, residual_out, direction_out
):
    total = jnp.sum(parts[...], axis=0)
    norm_now, curvature, cross, quad = (total[:, n : n + 1] for n in range(4))
    step = norm_now / curvature
    norm_next = norm_now - 2.0 * step * cross + step * step * quad
    ratio = norm_next / norm_now
    direction = smooth[...]
    res = residual[...] - step * applied[...]
    solution_out[...] = solution[...] + step * direction
    residual_out[...] = res
    direction_out[...] = res * inverse[...] + ratio * direction


def call(kernel, shapes, *args):
    outs = tuple(jax.ShapeDtypeStruct(shape, jnp.float32) for shape in shapes)
    vmem = pl.BlockSpec(memory_space=pltpu.VMEM)
    return pl.pallas_call(
        kernel,
        out_shape=outs,
        in_specs=[vmem] * len(args),
        out_specs=(vmem,) * len(outs),
        compiler_params=pltpu.CompilerParams(vmem_limit_bytes=8 * 2**20),
    )(*args)


def both_ways(low, high, axis):
    peers = lax.axis_size(axis)
    up = [(i, (i + 1) % peers) for i in range(peers)]
    before = lax.ppermute(high, axis, up)
    after = lax.ppermute(low, axis, [(j, i) for i, j in up])
    return before, after


def solution(mesh):
    groups = mesh.shape["group"]
    devs = mesh.shape["dev"]

    def on_device(solution, residual, direction, geometry, mass):
        local = solution.shape
        dims = local[1:3]
        rows = dims[0] * dims[1]
        points = local[3]
        flat = (rows, points)
        face_dev = (dims[1], LANES)
        face_group = (rows, LANES)
        solution, residual, direction, mass = (
            array.reshape(flat) for array in (solution, residual, direction, mass)
        )
        geometry = geometry.reshape((3,) + flat)
        tables = jnp.asarray(lane_tables())

        def bind(kernel):
            def body(*refs):
                kernel(dims, *refs)

            body.__name__ = kernel.__name__
            return body

        corners = bind(corner_kernel)
        field, dev_low, dev_high, group_low, group_high = call(
            bind(start_kernel),
            [flat, face_dev, face_dev, face_group, face_group],
            direction,
        )
        dev = both_ways(dev_low, dev_high, "dev")
        diag, tables, plane = call(
            bind(diagonal_kernel),
            [flat, tables.shape, (LANES, 2 * LANES)],
            geometry,
            mass,
            tables,
        )
        low, high = call(corners, [face_group] * 2, group_low, group_high, *dev)
        group = both_ways(low, high, "group")
        smooth, applied, dev_low, dev_high, group_low, group_high = call(
            bind(operator_kernel),
            [flat, flat, face_dev, face_dev, face_group, face_group],
            field,
            *dev,
            *group,
            geometry,
            mass,
            tables,
            plane,
            diag,
        )
        dev = both_ways(dev_low, dev_high, "dev")
        low, high = call(corners, [face_group] * 2, group_low, group_high, *dev)
        group = both_ways(low, high, "group")
        applied, inverse, sums = call(
            bind(products_kernel),
            [flat, flat, (groups, 1, LANES)],
            applied,
            diag,
            *dev,
            *group,
            residual,
            smooth,
        )
        sums = lax.all_to_all(sums, "group", 0, 0)
        (sums,) = call(middle_kernel, [(devs, 1, LANES)], sums)
        sums = lax.all_to_all(sums, "dev", 0, 0)
        outs = call(
            final_kernel, [flat] * 3, sums, solution, residual, smooth, applied, inverse
        )
        return tuple(out.reshape(local) for out in outs)

    spec = P("group", "dev", None, None)
    return jax.shard_map(
        on_device,
        mesh=mesh,
        in_specs=(spec, spec, spec, P(None, "group", "dev", None, None), spec),
        out_specs=(spec, spec, spec),
        check_vma=False,
    )
```

```python
import jax
import jax.numpy as jnp
import numpy as np
from jax import lax
from jax.experimental import pallas as pl
from jax.experimental.pallas import tpu as pltpu
from jax.sharding import PartitionSpec as P

NP = 8
LANES = 128
TILES = NP**3 // LANES
HALF = NP * NP
SECOND = 64
VMEM_BYTES = 8 * 2**20

lobatto_nodes = [
    -1.0,
    -0.8717401485096066,
    -0.5917001814331423,
    -0.2092992179024789,
    0.2092992179024789,
    0.5917001814331423,
    0.8717401485096066,
    1.0,
]


def derivative_table():
    nodes = np.array(lobatto_nodes)
    identity = np.eye(NP)
    offset = nodes[:, None] - nodes[None, :] + identity
    barycentric = 1.0 / np.prod(offset, axis=1)
    derivative = barycentric[None, :] / barycentric[:, None] / offset * (1.0 - identity)
    return derivative - identity * np.sum(derivative, axis=1)[:, None]


def lane_tables():
    derivative = derivative_table()
    half = np.arange(LANES) // HALF
    rows = []
    for matrix in (derivative, derivative.T):
        for out in range(TILES):
            for inp in range(TILES):
                rows.append(matrix[2 * out + half, 2 * inp + half])
                rows.append(matrix[2 * out + half, 2 * inp + 1 - half])
    lane = np.arange(LANES)
    rows.extend(derivative[(lane // NP) % NP, node] for node in range(NP))
    rows.extend(derivative[lane % NP, node] for node in range(NP))
    return np.stack(rows).astype(np.float32)


def lanes(rows):
    return lax.broadcasted_iota(jnp.int32, (rows, LANES), 1)


def plane_table(tables):
    lane = lanes(NP)
    sub = lax.broadcasted_iota(jnp.int32, (NP, LANES), 0)
    same_k = lane % NP == sub
    along_k = tables[SECOND + NP : SECOND + 2 * NP, :]
    parts_j, parts_k = [], []
    for block in range(LANES // NP):
        half, j = divmod(block, NP)
        along_j = jnp.broadcast_to(tables[SECOND + j : SECOND + j + 1, :], (NP, LANES))
        parts_j.append(jnp.where(same_k & (lane // HALF == half), along_j, 0.0))
        parts_k.append(jnp.where(lane // NP == block, along_k, 0.0))
    return jnp.concatenate(
        [jnp.concatenate(parts_j, axis=0), jnp.concatenate(parts_k, axis=0)], axis=1
    )


def lane_weights(tile):
    lane = lanes(1)
    i = 2 * tile + lane // HALF
    weight = jnp.ones((1, LANES), jnp.float32)
    for node in (i, (lane // NP) % NP, lane % NP):
        weight = weight * jnp.where((node == 0) | (node == NP - 1), 0.5, 1.0)
    return weight


def roll(value, shift, axis):
    return pltpu.roll(value, shift % value.shape[axis], axis)


def split(value, dims):
    eb, ez = dims
    return [
        [value[b * ez : (b + 1) * ez, t * LANES : (t + 1) * LANES] for b in range(eb)]
        for t in range(TILES)
    ]


def join(blocks):
    return jnp.concatenate([jnp.concatenate(tile, axis=0) for tile in blocks], axis=1)


def local_assemble(blocks):
    result = []
    for tile in blocks:
        lane = lanes(tile[0].shape[0])
        k = lane % NP
        j = (lane // NP) % NP
        summed = []
        for x in tile:
            above = roll(roll(x, NP - 1, 1), -1, 0)
            below = roll(roll(x, 1 - NP, 1), 1, 0)
            summed.append(x + jnp.where(k == NP - 1, above, jnp.where(k == 0, below, 0.0)))
        out = []
        last = len(summed) - 1
        for b, x in enumerate(summed):
            y = x
            if b < last:
                y = y + jnp.where(j == NP - 1, roll(summed[b + 1], HALF - NP, 1), 0.0)
            if b > 0:
                y = y + jnp.where(j == 0, roll(summed[b - 1], NP - HALF, 1), 0.0)
            out.append(y)
        result.append(out)
    return result


def pack_dev(fields, block, node):
    rows = fields[0][0][block].shape[0]
    lane = lanes(rows)
    packed = jnp.zeros((rows, LANES), jnp.float32)
    for f, blocks in enumerate(fields):
        for i in range(NP):
            t, h = divmod(i, 2)
            target = f * HALF + i * NP
            source = h * HALF + node * NP
            moved = roll(blocks[t][block], target - source, 1)
            packed = jnp.where(lane // NP == target // NP, moved, packed)
    return packed


def unpack_dev(packed, field, node, tile):
    lane = lanes(packed.shape[0])
    result = jnp.zeros(packed.shape, jnp.float32)
    for h in range(2):
        source = field * HALF + (2 * tile + h) * NP
        target = h * HALF + node * NP
        result = jnp.where(lane // NP == target // NP, roll(packed, target - source, 1), result)
    return result


def pack_group(fields, upper):
    tile = TILES - 1 if upper else 0
    parts = [jnp.concatenate(blocks[tile], axis=0) for blocks in fields]
    lane = lanes(parts[0].shape[0])
    if upper:
        parts[0] = roll(parts[0], HALF, 1)
    else:
        parts[1:] = [roll(part, HALF, 1) for part in parts[1:]]
    other = parts[1] if len(parts) > 1 else 0.0
    return jnp.where(lane < HALF, parts[0], other)


def add_dev(blocks, field, before, after):
    out = []
    for t, tile in enumerate(blocks):
        tile = list(tile)
        tile[0] = tile[0] + unpack_dev(before, field, 0, t)
        tile[-1] = tile[-1] + unpack_dev(after, field, NP - 1, t)
        out.append(tile)
    return out


def add_group(blocks, field, before, after):
    eb = len(blocks[0])
    ez = blocks[0][0].shape[0]
    lane = lanes(ez)
    out = [list(tile) for tile in blocks]
    for b in range(eb):
        low = before[b * ez : (b + 1) * ez, :]
        high = after[b * ez : (b + 1) * ez, :]
        if field:
            low = roll(low, HALF, 1)
        else:
            high = roll(high, HALF, 1)
        out[0][b] = out[0][b] + jnp.where(lane < HALF, low, 0.0)
        out[-1][b] = out[-1][b] + jnp.where(lane >= HALF, high, 0.0)
    return out


def first_direction(tables, base, tiles, squared=False):
    swapped = [roll(tile, HALF, 1) for tile in tiles]
    out = []
    for o in range(TILES):
        acc = None
        for i in range(TILES):
            row = base + 2 * (o * TILES + i)
            same = tables[row : row + 1, :]
            other = tables[row + 1 : row + 2, :]
            if squared:
                same, other = same * same, other * other
            term = same * tiles[i] + other * swapped[i]
            acc = term if acc is None else acc + term
        out.append(acc)
    return out


def halves(value):
    high = value.astype(jnp.bfloat16)
    return high, (value - high.astype(jnp.float32)).astype(jnp.bfloat16)


def matmul(lefts, rights, transposed=False):
    dims = (((1,), (1 if transposed else 0,)), ((), ()))
    total = None
    for n, left in enumerate(lefts):
        for right in rights[: len(rights) - n]:
            term = lax.dot_general(left, right, dims, preferred_element_type=jnp.float32)
            total = term if total is None else total + term
    return total


def tiles_of(value):
    return [value[:, t * LANES : (t + 1) * LANES] for t in range(TILES)]


def stack_rows(tiles):
    return jnp.concatenate(tiles, axis=0)


def unstack_rows(value):
    rows = value.shape[0] // TILES
    return [value[t * rows : (t + 1) * rows, :] for t in range(TILES)]


def blocks_of(tiles, dims):
    eb, ez = dims
    return [[tile[b * ez : (b + 1) * ez, :] for b in range(eb)] for tile in tiles]


def start_kernel(dims, direction, field_out, dev_low, dev_high, group_low, group_high):
    weighted = [
        lane_weights(t) * direction[:, t * LANES : (t + 1) * LANES] for t in range(TILES)
    ]
    blocks = local_assemble(blocks_of(weighted, dims))
    field_out[...] = join(blocks)
    dev_low[...] = pack_dev([blocks], 0, 0)
    dev_high[...] = pack_dev([blocks], dims[0] - 1, NP - 1)
    group_low[...] = pack_group([blocks], False)
    group_high[...] = pack_group([blocks], True)


def diagonal_kernel(dims, geometry, mass, tables, diag_out, tables_out, high_out, low_out):
    first = first_direction(
        tables, 32, tiles_of(geometry[0].astype(jnp.float32)), squared=True
    )
    table = plane_table(tables)
    tables_out[...] = tables[...]
    high_out[...], low_out[...] = halves(table)
    pair = jnp.concatenate(
        [stack_rows(tiles_of(geometry[1])), stack_rows(tiles_of(geometry[2]))], axis=1
    )
    rest = unstack_rows(matmul([pair], halves(table * table), transposed=True))
    masses = tiles_of(mass[...].astype(jnp.float32))
    local = [a + b + c for a, b, c in zip(first, rest, masses)]
    diag_out[...] = join(local_assemble(blocks_of(local, dims)))


def corner_kernel(dims, dev_low, dev_high, before, after, low_out, high_out):
    eb, ez = dims
    i = (lanes(ez) // NP) % NP
    for ref, out, upper in ((dev_low, low_out, False), (dev_high, high_out, True)):
        start = (eb - 1) * ez if upper else 0
        low = before[start : start + ez, :]
        high = after[start : start + ez, :]
        if upper:
            low = roll(low, NP - HALF, 1)
        else:
            high = roll(high, HALF - NP, 1)
        out[...] = ref[...] + jnp.where(i == 0, low, jnp.where(i == NP - 1, high, 0.0))


def operator_kernel(
    dims,
    field,
    dev_before,
    dev_after,
    group_before,
    group_after,
    geometry,
    mass,
    tables,
    plane_high,
    plane_low,
    diag,
    smooth_out,
    applied_out,
    dev_low,
    dev_high,
    group_low,
    group_high,
):
    blocks = split(field, dims)
    blocks = add_dev(blocks, 0, dev_before[...], dev_after[...])
    blocks = add_group(blocks, 0, group_before, group_after)
    smooth_out[...] = join(blocks)
    tiles = [jnp.concatenate(tile, axis=0) for tile in blocks]
    geo = [tiles_of(geometry[c].astype(jnp.float32)) for c in range(3)]
    table = (plane_high[...], plane_low[...])
    first = [g * f for g, f in zip(geo[0], first_direction(tables, 0, tiles))]
    gradient = matmul(halves(stack_rows(tiles)), table)
    pair = jnp.concatenate([stack_rows(geo[1]), stack_rows(geo[2])], axis=1) * gradient
    rest = unstack_rows(matmul(halves(pair), table, transposed=True))
    first = first_direction(tables, 32, first)
    masses = tiles_of(mass[...].astype(jnp.float32))
    local = [a + b + m * u for a, b, m, u in zip(first, rest, masses, tiles)]
    blocks = local_assemble(blocks_of(local, dims))
    applied_out[...] = join(blocks)
    diag_blocks = split(diag, dims)
    dev_low[...] = pack_dev([blocks, diag_blocks], 0, 0)
    dev_high[...] = pack_dev([blocks, diag_blocks], dims[0] - 1, NP - 1)
    group_low[...] = pack_group([blocks, diag_blocks], False)
    group_high[...] = pack_group([blocks, diag_blocks], True)


def products_kernel(
    dims,
    field,
    diag,
    dev_before,
    dev_after,
    group_before,
    group_after,
    residual,
    smooth,
    applied_out,
    inverse_out,
    sums_out,
):
    full = []
    for index, ref in enumerate((field, diag)):
        blocks = add_dev(split(ref, dims), index, dev_before[...], dev_after[...])
        blocks = add_group(blocks, index, group_before, group_after)
        full.append([jnp.concatenate(tile, axis=0) for tile in blocks])
    sums = [None] * 4
    for t in range(TILES):
        window = slice(t * LANES, (t + 1) * LANES)
        weight = lane_weights(t)
        applied = full[0][t]
        inverse = 1.0 / full[1][t]
        applied_out[:, window] = applied
        inverse_out[:, window] = inverse
        res = residual[:, window]
        weighted = weight * inverse
        terms = (
            weighted * res * res,
            weight * smooth[:, window] * applied,
            weighted * res * applied,
            weighted * applied * applied,
        )
        sums = [term if s is None else s + term for s, term in zip(sums, terms)]
    lane = lanes(1)
    row = jnp.zeros((1, LANES), jnp.float32)
    for n, total in enumerate(sums):
        column = jnp.sum(total, axis=0, keepdims=True)
        row = jnp.where(lane == n, jnp.sum(column, axis=1, keepdims=True), row)
    sums_out[...] = jnp.broadcast_to(row.reshape(1, 1, LANES), sums_out.shape)


def middle_kernel(parts, sums_out):
    total = jnp.sum(parts[...], axis=0, keepdims=True)
    sums_out[...] = jnp.broadcast_to(total, sums_out.shape)


def final_kernel(parts, solution, residual, smooth, applied, inverse, *refs):
    targets, buffers, sems = refs[:3], refs[3:6], refs[6]
    copies = [
        pltpu.make_async_copy(source, target, sems.at[n])
        for n, (source, target) in enumerate(zip(buffers, targets))
    ]
    total = jnp.sum(parts[...], axis=0)
    norm_now, curvature, cross, quad = (total[:, n : n + 1] for n in range(4))
    step = norm_now / curvature
    direction = smooth[...]
    buffers[0][...] = solution[...] + step * direction
    copies[0].start()
    res = residual[...] - step * applied[...]
    buffers[1][...] = res
    copies[1].start()
    norm_next = norm_now - 2.0 * step * cross + step * step * quad
    buffers[2][...] = res * inverse[...] + (norm_next / norm_now) * direction
    copies[2].start()
    for copy in copies:
        copy.wait()


def call(kernel, shapes, *args):
    typed = [s if isinstance(s[1], type) else (s, jnp.float32) for s in shapes]
    outs = tuple(jax.ShapeDtypeStruct(shape, dtype) for shape, dtype in typed)
    vmem = pl.BlockSpec(memory_space=pltpu.VMEM)
    return pl.pallas_call(
        kernel,
        out_shape=outs,
        in_specs=[vmem] * len(args),
        out_specs=(vmem,) * len(outs),
        compiler_params=pltpu.CompilerParams(vmem_limit_bytes=VMEM_BYTES),
    )(*args)


def both_ways(low, high, axis):
    peers = lax.axis_size(axis)
    up = [(i, (i + 1) % peers) for i in range(peers)]
    before = lax.ppermute(high, axis, up)
    after = lax.ppermute(low, axis, [(j, i) for i, j in up])
    return before, after


def solution(mesh):
    groups = mesh.shape["group"]
    devs = mesh.shape["dev"]

    def on_device(solution, residual, direction, geometry, mass):
        local = solution.shape
        dims = local[1:3]
        rows = dims[0] * dims[1]
        points = local[3]
        flat = (rows, points)
        face_dev = (dims[1], LANES)
        face_group = (rows, LANES)
        solution, residual, direction, mass = (
            array.reshape(flat) for array in (solution, residual, direction, mass)
        )
        geometry = geometry.reshape((3,) + flat)
        tables = jnp.asarray(lane_tables())

        def bind(kernel):
            def body(*refs):
                kernel(dims, *refs)

            body.__name__ = kernel.__name__
            return body

        def exchange(dev_low, dev_high, group_low, group_high):
            group = both_ways(group_low, group_high, "group")
            faces = call(bind(corner_kernel), [face_dev] * 2, dev_low, dev_high, *group)
            return both_ways(*faces, "dev"), group

        field, dev_low, dev_high, group_low, group_high = call(
            bind(start_kernel),
            [flat, face_dev, face_dev, face_group, face_group],
            direction,
        )
        diag, tables, *plane = call(
            bind(diagonal_kernel),
            [flat, tables.shape] + [((LANES, 2 * LANES), jnp.bfloat16)] * 2,
            geometry,
            mass,
            tables,
        )
        dev, group = exchange(dev_low, dev_high, group_low, group_high)
        smooth, applied, dev_low, dev_high, group_low, group_high = call(
            bind(operator_kernel),
            [flat, flat, face_dev, face_dev, face_group, face_group],
            field,
            *dev,
            *group,
            geometry,
            mass,
            tables,
            *plane,
            diag,
        )
        dev, group = exchange(dev_low, dev_high, group_low, group_high)
        applied, inverse, sums = call(
            bind(products_kernel),
            [flat, flat, (groups, 1, LANES)],
            applied,
            diag,
            *dev,
            *group,
            residual,
            smooth,
        )
        sums = lax.all_to_all(sums, "group", 0, 0)
        (sums,) = call(middle_kernel, [(devs, 1, LANES)], sums)
        sums = lax.all_to_all(sums, "dev", 0, 0)
        outs = pl.pallas_call(
            final_kernel,
            out_shape=(jax.ShapeDtypeStruct(flat, jnp.float32),) * 3,
            in_specs=[pl.BlockSpec(memory_space=pltpu.VMEM)] * 6,
            out_specs=(pl.BlockSpec(memory_space=pltpu.HBM),) * 3,
            scratch_shapes=[pltpu.VMEM(flat, jnp.float32)] * 3 + [pltpu.SemaphoreType.DMA((3,))],
            compiler_params=pltpu.CompilerParams(vmem_limit_bytes=VMEM_BYTES),
        )(sums, solution, residual, smooth, applied, inverse)
        return tuple(out.reshape(local) for out in outs)

    spec = P("group", "dev", None, None)
    return jax.shard_map(
        on_device,
        mesh=mesh,
        in_specs=(spec, spec, spec, P(None, "group", "dev", None, None), spec),
        out_specs=(spec, spec, spec),
        check_vma=False,
    )
```

```python
import jax
import jax.numpy as jnp
import numpy as np
from jax import lax
from jax.experimental import pallas as pl
from jax.experimental.pallas import tpu as pltpu
from jax.sharding import PartitionSpec as P

NP = 8
LANES = 128
TILES = NP**3 // LANES
HALF = NP * NP
SECOND = 64
VMEM_BYTES = 8 * 2**20

lobatto_nodes = [
    -1.0,
    -0.8717401485096066,
    -0.5917001814331423,
    -0.2092992179024789,
    0.2092992179024789,
    0.5917001814331423,
    0.8717401485096066,
    1.0,
]


def derivative_table():
    nodes = np.array(lobatto_nodes)
    identity = np.eye(NP)
    offset = nodes[:, None] - nodes[None, :] + identity
    barycentric = 1.0 / np.prod(offset, axis=1)
    derivative = barycentric[None, :] / barycentric[:, None] / offset * (1.0 - identity)
    return derivative - identity * np.sum(derivative, axis=1)[:, None]


def lane_tables():
    derivative = derivative_table()
    half = np.arange(LANES) // HALF
    rows = []
    for matrix in (derivative, derivative.T):
        for out in range(TILES):
            for inp in range(TILES):
                rows.append(matrix[2 * out + half, 2 * inp + half])
                rows.append(matrix[2 * out + half, 2 * inp + 1 - half])
    lane = np.arange(LANES)
    rows.extend(derivative[(lane // NP) % NP, node] for node in range(NP))
    rows.extend(derivative[lane % NP, node] for node in range(NP))
    return np.stack(rows).astype(np.float32)


def lanes(rows):
    return lax.broadcasted_iota(jnp.int32, (rows, LANES), 1)


def plane_table(tables):
    lane = lanes(NP)
    sub = lax.broadcasted_iota(jnp.int32, (NP, LANES), 0)
    same_k = lane % NP == sub
    along_k = tables[SECOND + NP : SECOND + 2 * NP, :]
    parts_j, parts_k = [], []
    for block in range(LANES // NP):
        half, j = divmod(block, NP)
        along_j = jnp.broadcast_to(tables[SECOND + j : SECOND + j + 1, :], (NP, LANES))
        parts_j.append(jnp.where(same_k & (lane // HALF == half), along_j, 0.0))
        parts_k.append(jnp.where(lane // NP == block, along_k, 0.0))
    return jnp.concatenate(
        [jnp.concatenate(parts_j, axis=0), jnp.concatenate(parts_k, axis=0)], axis=1
    )


def lane_weights(tile):
    lane = lanes(1)
    i = 2 * tile + lane // HALF
    weight = jnp.ones((1, LANES), jnp.float32)
    for node in (i, (lane // NP) % NP, lane % NP):
        weight = weight * jnp.where((node == 0) | (node == NP - 1), 0.5, 1.0)
    return weight


def roll(value, shift, axis):
    return pltpu.roll(value, shift % value.shape[axis], axis)


def split(value, dims):
    eb, ez = dims
    return [
        [value[b * ez : (b + 1) * ez, t * LANES : (t + 1) * LANES] for b in range(eb)]
        for t in range(TILES)
    ]


def join(blocks):
    return jnp.concatenate([jnp.concatenate(tile, axis=0) for tile in blocks], axis=1)


def local_assemble(blocks):
    result = []
    for tile in blocks:
        lane = lanes(tile[0].shape[0])
        k = lane % NP
        j = (lane // NP) % NP
        summed = []
        for x in tile:
            above = roll(roll(x, NP - 1, 1), -1, 0)
            below = roll(roll(x, 1 - NP, 1), 1, 0)
            summed.append(x + jnp.where(k == NP - 1, above, jnp.where(k == 0, below, 0.0)))
        out = []
        last = len(summed) - 1
        for b, x in enumerate(summed):
            y = x
            if b < last:
                y = y + jnp.where(j == NP - 1, roll(summed[b + 1], HALF - NP, 1), 0.0)
            if b > 0:
                y = y + jnp.where(j == 0, roll(summed[b - 1], NP - HALF, 1), 0.0)
            out.append(y)
        result.append(out)
    return result


def pack_dev(fields, block, node):
    rows = fields[0][0][block].shape[0]
    lane = lanes(rows)
    packed = jnp.zeros((rows, LANES), jnp.float32)
    for f, blocks in enumerate(fields):
        for i in range(NP):
            t, h = divmod(i, 2)
            target = f * HALF + i * NP
            source = h * HALF + node * NP
            moved = roll(blocks[t][block], target - source, 1)
            packed = jnp.where(lane // NP == target // NP, moved, packed)
    return packed


def unpack_dev(packed, field, node, tile):
    lane = lanes(packed.shape[0])
    result = jnp.zeros(packed.shape, jnp.float32)
    for h in range(2):
        source = field * HALF + (2 * tile + h) * NP
        target = h * HALF + node * NP
        result = jnp.where(lane // NP == target // NP, roll(packed, target - source, 1), result)
    return result


def pack_group(fields, upper):
    tile = TILES - 1 if upper else 0
    parts = [jnp.concatenate(blocks[tile], axis=0) for blocks in fields]
    lane = lanes(parts[0].shape[0])
    if upper:
        parts[0] = roll(parts[0], HALF, 1)
    else:
        parts[1:] = [roll(part, HALF, 1) for part in parts[1:]]
    other = parts[1] if len(parts) > 1 else 0.0
    return jnp.where(lane < HALF, parts[0], other)


def add_dev(blocks, field, before, after):
    out = []
    for t, tile in enumerate(blocks):
        tile = list(tile)
        tile[0] = tile[0] + unpack_dev(before, field, 0, t)
        tile[-1] = tile[-1] + unpack_dev(after, field, NP - 1, t)
        out.append(tile)
    return out


def add_group(blocks, field, before, after):
    eb = len(blocks[0])
    ez = blocks[0][0].shape[0]
    lane = lanes(ez)
    out = [list(tile) for tile in blocks]
    for b in range(eb):
        low = before[b * ez : (b + 1) * ez, :]
        high = after[b * ez : (b + 1) * ez, :]
        if field:
            low = roll(low, HALF, 1)
        else:
            high = roll(high, HALF, 1)
        out[0][b] = out[0][b] + jnp.where(lane < HALF, low, 0.0)
        out[-1][b] = out[-1][b] + jnp.where(lane >= HALF, high, 0.0)
    return out


def first_direction(tables, base, tiles, squared=False):
    swapped = [roll(tile, HALF, 1) for tile in tiles]
    out = []
    for o in range(TILES):
        acc = None
        for i in range(TILES):
            row = base + 2 * (o * TILES + i)
            same = tables[row : row + 1, :]
            other = tables[row + 1 : row + 2, :]
            if squared:
                same, other = same * same, other * other
            term = same * tiles[i] + other * swapped[i]
            acc = term if acc is None else acc + term
        out.append(acc)
    return out


def halves(value):
    high = value.astype(jnp.bfloat16)
    return high, (value - high.astype(jnp.float32)).astype(jnp.bfloat16)


def matmul(lefts, rights, transposed=False):
    dims = (((1,), (1 if transposed else 0,)), ((), ()))
    total = None
    for n, left in enumerate(lefts):
        for right in rights[: len(rights) - n]:
            term = lax.dot_general(left, right, dims, preferred_element_type=jnp.float32)
            total = term if total is None else total + term
    return total


def tiles_of(value):
    return [value[:, t * LANES : (t + 1) * LANES] for t in range(TILES)]


def stack_rows(tiles):
    return jnp.concatenate(tiles, axis=0)


def unstack_rows(value):
    rows = value.shape[0] // TILES
    return [value[t * rows : (t + 1) * rows, :] for t in range(TILES)]


def blocks_of(tiles, dims):
    eb, ez = dims
    return [[tile[b * ez : (b + 1) * ez, :] for b in range(eb)] for tile in tiles]


def start_kernel(dims, direction, field_out, dev_low, dev_high, group_low, group_high):
    weighted = [
        lane_weights(t) * direction[:, t * LANES : (t + 1) * LANES] for t in range(TILES)
    ]
    blocks = local_assemble(blocks_of(weighted, dims))
    field_out[...] = join(blocks)
    dev_low[...] = pack_dev([blocks], 0, 0)
    dev_high[...] = pack_dev([blocks], dims[0] - 1, NP - 1)
    group_low[...] = pack_group([blocks], False)
    group_high[...] = pack_group([blocks], True)


def diagonal_kernel(dims, geometry, mass, tables, diag_out, tables_out, high_out, low_out):
    first = first_direction(
        tables, 32, tiles_of(geometry[0].astype(jnp.float32)), squared=True
    )
    table = plane_table(tables)
    tables_out[...] = tables[...]
    high_out[...], low_out[...] = halves(table)
    pair = jnp.concatenate(
        [stack_rows(tiles_of(geometry[1])), stack_rows(tiles_of(geometry[2]))], axis=1
    )
    rest = unstack_rows(matmul([pair], halves(table * table), transposed=True))
    masses = tiles_of(mass[...].astype(jnp.float32))
    local = [a + b + c for a, b, c in zip(first, rest, masses)]
    diag_out[...] = join(local_assemble(blocks_of(local, dims)))


def corner_kernel(dims, dev_low, dev_high, before, after, ready, low_out, high_out):
    eb, ez = dims
    i = (lanes(ez) // NP) % NP
    for ref, out, upper in ((dev_low, low_out, False), (dev_high, high_out, True)):
        start = (eb - 1) * ez if upper else 0
        low = before[start : start + ez, :]
        high = after[start : start + ez, :]
        if upper:
            low = roll(low, NP - HALF, 1)
        else:
            high = roll(high, HALF - NP, 1)
        out[...] = ref[...] + jnp.where(i == 0, low, jnp.where(i == NP - 1, high, 0.0))


def operator_kernel(
    dims,
    field,
    dev_before,
    dev_after,
    group_before,
    group_after,
    geometry,
    mass,
    tables,
    plane_high,
    plane_low,
    diag,
    smooth_out,
    applied_out,
    dev_low,
    dev_high,
    group_low,
    group_high,
):
    blocks = split(field, dims)
    blocks = add_dev(blocks, 0, dev_before[...], dev_after[...])
    blocks = add_group(blocks, 0, group_before, group_after)
    smooth_out[...] = join(blocks)
    tiles = [jnp.concatenate(tile, axis=0) for tile in blocks]
    geo = [tiles_of(geometry[c].astype(jnp.float32)) for c in range(3)]
    table = (plane_high[...], plane_low[...])
    first = [g * f for g, f in zip(geo[0], first_direction(tables, 0, tiles))]
    gradient = matmul(halves(stack_rows(tiles)), table)
    pair = jnp.concatenate([stack_rows(geo[1]), stack_rows(geo[2])], axis=1) * gradient
    rest = unstack_rows(matmul(halves(pair), table, transposed=True))
    first = first_direction(tables, 32, first)
    masses = tiles_of(mass[...].astype(jnp.float32))
    local = [a + b + m * u for a, b, m, u in zip(first, rest, masses, tiles)]
    blocks = local_assemble(blocks_of(local, dims))
    applied_out[...] = join(blocks)
    diag_blocks = split(diag, dims)
    dev_low[...] = pack_dev([blocks, diag_blocks], 0, 0)
    dev_high[...] = pack_dev([blocks, diag_blocks], dims[0] - 1, NP - 1)
    group_low[...] = pack_group([blocks, diag_blocks], False)
    group_high[...] = pack_group([blocks, diag_blocks], True)


def products_kernel(
    dims,
    field,
    diag,
    dev_before,
    dev_after,
    group_before,
    group_after,
    residual,
    smooth,
    applied_out,
    inverse_out,
    sums_out,
):
    full = []
    for index, ref in enumerate((field, diag)):
        blocks = add_dev(split(ref, dims), index, dev_before[...], dev_after[...])
        blocks = add_group(blocks, index, group_before, group_after)
        full.append([jnp.concatenate(tile, axis=0) for tile in blocks])
    sums = [None] * 4
    for t in range(TILES):
        window = slice(t * LANES, (t + 1) * LANES)
        weight = lane_weights(t)
        applied = full[0][t]
        inverse = 1.0 / full[1][t]
        applied_out[:, window] = applied
        inverse_out[:, window] = inverse
        res = residual[:, window]
        weighted = weight * inverse
        terms = (
            weighted * res * res,
            weight * smooth[:, window] * applied,
            weighted * res * applied,
            weighted * applied * applied,
        )
        sums = [term if s is None else s + term for s, term in zip(sums, terms)]
    lane = lanes(1)
    row = jnp.zeros((1, LANES), jnp.float32)
    for n, total in enumerate(sums):
        column = jnp.sum(total, axis=0, keepdims=True)
        row = jnp.where(lane == n, jnp.sum(column, axis=1, keepdims=True), row)
    sums_out[...] = jnp.broadcast_to(row.reshape(1, 1, LANES), sums_out.shape)


def middle_kernel(parts, sums_out):
    total = jnp.sum(parts[...], axis=0, keepdims=True)
    sums_out[...] = jnp.broadcast_to(total, sums_out.shape)


def final_kernel(
    parts, solution, residual, smooth, applied, inverse, solution_out, residual_out, direction_out
):
    total = jnp.sum(parts[...], axis=0)
    norm_now, curvature, cross, quad = (total[:, n : n + 1] for n in range(4))
    step = norm_now / curvature
    norm_next = norm_now - 2.0 * step * cross + step * step * quad
    ratio = norm_next / norm_now
    direction = smooth[...]
    res = residual[...] - step * applied[...]
    solution_out[...] = solution[...] + step * direction
    residual_out[...] = res
    direction_out[...] = res * inverse[...] + ratio * direction


def call(kernel, shapes, *args):
    typed = [s if isinstance(s[1], type) else (s, jnp.float32) for s in shapes]
    outs = tuple(jax.ShapeDtypeStruct(shape, dtype) for shape, dtype in typed)
    vmem = pl.BlockSpec(memory_space=pltpu.VMEM)
    return pl.pallas_call(
        kernel,
        out_shape=outs,
        in_specs=[vmem] * len(args),
        out_specs=(vmem,) * len(outs),
        compiler_params=pltpu.CompilerParams(vmem_limit_bytes=VMEM_BYTES),
    )(*args)


def both_ways(low, high, axis):
    peers = lax.axis_size(axis)
    up = [(i, (i + 1) % peers) for i in range(peers)]
    before = lax.ppermute(high, axis, up)
    after = lax.ppermute(low, axis, [(j, i) for i, j in up])
    return before, after


def solution(mesh):
    groups = mesh.shape["group"]
    devs = mesh.shape["dev"]

    def on_device(solution, residual, direction, geometry, mass):
        local = solution.shape
        dims = local[1:3]
        rows = dims[0] * dims[1]
        points = local[3]
        flat = (rows, points)
        face_dev = (dims[1], LANES)
        face_group = (rows, LANES)
        solution, residual, direction, mass = (
            array.reshape(flat) for array in (solution, residual, direction, mass)
        )
        geometry = geometry.reshape((3,) + flat)
        tables = jnp.asarray(lane_tables())

        def bind(kernel):
            def body(*refs):
                kernel(dims, *refs)

            body.__name__ = kernel.__name__
            return body

        def exchange(dev_low, dev_high, group_low, group_high, ready):
            group = both_ways(group_low, group_high, "group")
            faces = call(
                bind(corner_kernel), [face_dev] * 2, dev_low, dev_high, *group, ready
            )
            return both_ways(*faces, "dev"), group

        field, dev_low, dev_high, group_low, group_high = call(
            bind(start_kernel),
            [flat, face_dev, face_dev, face_group, face_group],
            direction,
        )
        diag, tables, *plane = call(
            bind(diagonal_kernel),
            [flat, tables.shape] + [((LANES, 2 * LANES), jnp.bfloat16)] * 2,
            geometry,
            mass,
            tables,
        )
        dev, group = exchange(dev_low, dev_high, group_low, group_high, tables)
        smooth, applied, dev_low, dev_high, group_low, group_high = call(
            bind(operator_kernel),
            [flat, flat, face_dev, face_dev, face_group, face_group],
            field,
            *dev,
            *group,
            geometry,
            mass,
            tables,
            *plane,
            diag,
        )
        dev, group = exchange(dev_low, dev_high, group_low, group_high, tables)
        applied, inverse, sums = call(
            bind(products_kernel),
            [flat, flat, (groups, 1, LANES)],
            applied,
            diag,
            *dev,
            *group,
            residual,
            smooth,
        )
        sums = lax.all_to_all(sums, "group", 0, 0)
        (sums,) = call(middle_kernel, [(devs, 1, LANES)], sums)
        sums = lax.all_to_all(sums, "dev", 0, 0)
        outs = call(
            final_kernel, [flat] * 3, sums, solution, residual, smooth, applied, inverse
        )
        return tuple(out.reshape(local) for out in outs)

    spec = P("group", "dev", None, None)
    return jax.shard_map(
        on_device,
        mesh=mesh,
        in_specs=(spec, spec, spec, P(None, "group", "dev", None, None), spec),
        out_specs=(spec, spec, spec),
        check_vma=False,
    )
```

```python
import jax
import jax.numpy as jnp
import numpy as np
from jax import lax
from jax.experimental import pallas as pl
from jax.experimental.pallas import tpu as pltpu
from jax.sharding import PartitionSpec as P

NP = 8
LANES = 128
TILES = NP**3 // LANES
HALF = NP * NP
SECOND = 64
ORDERS = ("dev", "group")

lobatto_nodes = [
    -1.0,
    -0.8717401485096066,
    -0.5917001814331423,
    -0.2092992179024789,
    0.2092992179024789,
    0.5917001814331423,
    0.8717401485096066,
    1.0,
]


def derivative_table():
    nodes = np.array(lobatto_nodes)
    identity = np.eye(NP)
    offset = nodes[:, None] - nodes[None, :] + identity
    barycentric = 1.0 / np.prod(offset, axis=1)
    derivative = barycentric[None, :] / barycentric[:, None] / offset * (1.0 - identity)
    return derivative - identity * np.sum(derivative, axis=1)[:, None]


def lane_tables():
    derivative = derivative_table()
    half = np.arange(LANES) // HALF
    rows = []
    for matrix in (derivative, derivative.T):
        for out in range(TILES):
            for inp in range(TILES):
                rows.append(matrix[2 * out + half, 2 * inp + half])
                rows.append(matrix[2 * out + half, 2 * inp + 1 - half])
    lane = np.arange(LANES)
    rows.extend(derivative[(lane // NP) % NP, node] for node in range(NP))
    rows.extend(derivative[lane % NP, node] for node in range(NP))
    return np.stack(rows).astype(np.float32)


def lanes(rows):
    return lax.broadcasted_iota(jnp.int32, (rows, LANES), 1)


def plane_table(tables):
    lane = lanes(NP)
    sub = lax.broadcasted_iota(jnp.int32, (NP, LANES), 0)
    same_k = lane % NP == sub
    along_k = tables[SECOND + NP : SECOND + 2 * NP, :]
    parts_j, parts_k = [], []
    for block in range(LANES // NP):
        half, j = divmod(block, NP)
        along_j = jnp.broadcast_to(tables[SECOND + j : SECOND + j + 1, :], (NP, LANES))
        parts_j.append(jnp.where(same_k & (lane // HALF == half), along_j, 0.0))
        parts_k.append(jnp.where(lane // NP == block, along_k, 0.0))
    return jnp.concatenate(
        [jnp.concatenate(parts_j, axis=0), jnp.concatenate(parts_k, axis=0)], axis=1
    )


def lane_weights(tile):
    lane = lanes(1)
    i = 2 * tile + lane // HALF
    weight = jnp.ones((1, LANES), jnp.float32)
    for node in (i, (lane // NP) % NP, lane % NP):
        weight = weight * jnp.where((node == 0) | (node == NP - 1), 0.5, 1.0)
    return weight


def roll(value, shift, axis):
    return pltpu.roll(value, shift % value.shape[axis], axis)


def split(value, dims):
    eb, ez = dims
    return [
        [value[b * ez : (b + 1) * ez, t * LANES : (t + 1) * LANES] for b in range(eb)]
        for t in range(TILES)
    ]


def join(blocks):
    return jnp.concatenate([jnp.concatenate(tile, axis=0) for tile in blocks], axis=1)


def local_assemble(blocks):
    result = []
    for tile in blocks:
        lane = lanes(tile[0].shape[0])
        k = lane % NP
        j = (lane // NP) % NP
        summed = []
        for x in tile:
            above = roll(roll(x, NP - 1, 1), -1, 0)
            below = roll(roll(x, 1 - NP, 1), 1, 0)
            summed.append(x + jnp.where(k == NP - 1, above, jnp.where(k == 0, below, 0.0)))
        out = []
        last = len(summed) - 1
        for b, x in enumerate(summed):
            y = x
            if b < last:
                y = y + jnp.where(j == NP - 1, roll(summed[b + 1], HALF - NP, 1), 0.0)
            if b > 0:
                y = y + jnp.where(j == 0, roll(summed[b - 1], NP - HALF, 1), 0.0)
            out.append(y)
        result.append(out)
    return result


def pack_dev(fields, block, node):
    rows = fields[0][0][block].shape[0]
    lane = lanes(rows)
    packed = jnp.zeros((rows, LANES), jnp.float32)
    for f, blocks in enumerate(fields):
        for i in range(NP):
            t, h = divmod(i, 2)
            target = f * HALF + i * NP
            source = h * HALF + node * NP
            moved = roll(blocks[t][block], target - source, 1)
            packed = jnp.where(lane // NP == target // NP, moved, packed)
    return packed


def unpack_dev(packed, field, node, tile):
    lane = lanes(packed.shape[0])
    result = jnp.zeros(packed.shape, jnp.float32)
    for h in range(2):
        source = field * HALF + (2 * tile + h) * NP
        target = h * HALF + node * NP
        result = jnp.where(lane // NP == target // NP, roll(packed, target - source, 1), result)
    return result


def pack_group(fields, upper):
    tile = TILES - 1 if upper else 0
    parts = [jnp.concatenate(blocks[tile], axis=0) for blocks in fields]
    lane = lanes(parts[0].shape[0])
    if upper:
        parts[0] = roll(parts[0], HALF, 1)
    else:
        parts[1:] = [roll(part, HALF, 1) for part in parts[1:]]
    other = parts[1] if len(parts) > 1 else 0.0
    return jnp.where(lane < HALF, parts[0], other)


def add_dev(blocks, field, before, after):
    out = []
    for t, tile in enumerate(blocks):
        tile = list(tile)
        tile[0] = tile[0] + unpack_dev(before, field, 0, t)
        tile[-1] = tile[-1] + unpack_dev(after, field, NP - 1, t)
        out.append(tile)
    return out


def add_group(blocks, field, before, after):
    eb = len(blocks[0])
    ez = blocks[0][0].shape[0]
    lane = lanes(ez)
    out = [list(tile) for tile in blocks]
    for b in range(eb):
        low = before[b * ez : (b + 1) * ez, :]
        high = after[b * ez : (b + 1) * ez, :]
        if field:
            low = roll(low, HALF, 1)
        else:
            high = roll(high, HALF, 1)
        out[0][b] = out[0][b] + jnp.where(lane < HALF, low, 0.0)
        out[-1][b] = out[-1][b] + jnp.where(lane >= HALF, high, 0.0)
    return out


def first_direction(tables, base, tiles, squared=False):
    swapped = [roll(tile, HALF, 1) for tile in tiles]
    out = []
    for o in range(TILES):
        acc = None
        for i in range(TILES):
            row = base + 2 * (o * TILES + i)
            same = tables[row : row + 1, :]
            other = tables[row + 1 : row + 2, :]
            if squared:
                same, other = same * same, other * other
            term = same * tiles[i] + other * swapped[i]
            acc = term if acc is None else acc + term
        out.append(acc)
    return out


def halves(value):
    high = value.astype(jnp.bfloat16)
    return high, (value - high.astype(jnp.float32)).astype(jnp.bfloat16)


def matmul(lefts, rights, transposed=False):
    dims = (((1,), (1 if transposed else 0,)), ((), ()))
    total = None
    for n, left in enumerate(lefts):
        for right in rights[: len(rights) - n]:
            term = lax.dot_general(left, right, dims, preferred_element_type=jnp.float32)
            total = term if total is None else total + term
    return total


def tiles_of(value):
    return [value[:, t * LANES : (t + 1) * LANES] for t in range(TILES)]


def stack_rows(tiles):
    return jnp.concatenate(tiles, axis=0)


def unstack_rows(value):
    rows = value.shape[0] // TILES
    return [value[t * rows : (t + 1) * rows, :] for t in range(TILES)]


def blocks_of(tiles, dims):
    eb, ez = dims
    return [[tile[b * ez : (b + 1) * ez, :] for b in range(eb)] for tile in tiles]


def start_kernel(dims, direction, field_out, dev_low, dev_high, group_low, group_high):
    weighted = [
        lane_weights(t) * direction[:, t * LANES : (t + 1) * LANES] for t in range(TILES)
    ]
    blocks = local_assemble(blocks_of(weighted, dims))
    field_out[...] = join(blocks)
    dev_low[...] = pack_dev([blocks], 0, 0)
    dev_high[...] = pack_dev([blocks], dims[0] - 1, NP - 1)
    group_low[...] = pack_group([blocks], False)
    group_high[...] = pack_group([blocks], True)


def diagonal_kernel(dims, geometry, mass, tables, diag_out, tables_out, high_out, low_out):
    first = first_direction(
        tables, 32, tiles_of(geometry[0].astype(jnp.float32)), squared=True
    )
    table = plane_table(tables)
    tables_out[...] = tables[...]
    high_out[...], low_out[...] = halves(table)
    pair = jnp.concatenate(
        [stack_rows(tiles_of(geometry[1])), stack_rows(tiles_of(geometry[2]))], axis=1
    )
    rest = unstack_rows(matmul([pair], halves(table * table), transposed=True))
    masses = tiles_of(mass[...].astype(jnp.float32))
    local = [a + b + c for a, b, c in zip(first, rest, masses)]
    diag_out[...] = join(local_assemble(blocks_of(local, dims)))


def corner_kernel(dims, group_low, group_high, before, after, low_out, high_out):
    eb, ez = dims
    low_recv = before[...]
    high_recv = after[...]
    lane = lanes(ez)
    j = (lane // NP) % NP
    for ref, out, upper in ((group_low, low_out, False), (group_high, high_out, True)):
        shift_low = NP - HALF if upper else 0
        shift_high = 0 if upper else HALF - NP
        blocks = [ref[b * ez : (b + 1) * ez, :] for b in range(eb)]
        low = roll(low_recv, shift_low, 1) if shift_low else low_recv
        high = roll(high_recv, shift_high, 1) if shift_high else high_recv
        blocks[0] = blocks[0] + jnp.where(j == 0, low, 0.0)
        blocks[-1] = blocks[-1] + jnp.where(j == NP - 1, high, 0.0)
        for b in range(eb):
            out[b * ez : (b + 1) * ez, :] = blocks[b]


def corner_dev_kernel(dims, dev_low, dev_high, before, after, low_out, high_out):
    eb, ez = dims
    i = (lanes(ez) // NP) % NP
    for ref, out, upper in ((dev_low, low_out, False), (dev_high, high_out, True)):
        start = (eb - 1) * ez if upper else 0
        low = before[start : start + ez, :]
        high = after[start : start + ez, :]
        if upper:
            low = roll(low, NP - HALF, 1)
        else:
            high = roll(high, HALF - NP, 1)
        out[...] = ref[...] + jnp.where(i == 0, low, jnp.where(i == NP - 1, high, 0.0))


def operator_kernel(
    dims,
    field,
    dev_before,
    dev_after,
    group_before,
    group_after,
    geometry,
    mass,
    tables,
    plane_high,
    plane_low,
    diag,
    smooth_out,
    applied_out,
    dev_low,
    dev_high,
    group_low,
    group_high,
):
    blocks = split(field, dims)
    blocks = add_dev(blocks, 0, dev_before[...], dev_after[...])
    blocks = add_group(blocks, 0, group_before, group_after)
    smooth_out[...] = join(blocks)
    tiles = [jnp.concatenate(tile, axis=0) for tile in blocks]
    geo = [tiles_of(geometry[c].astype(jnp.float32)) for c in range(3)]
    table = (plane_high[...], plane_low[...])
    first = [g * f for g, f in zip(geo[0], first_direction(tables, 0, tiles))]
    gradient = matmul(halves(stack_rows(tiles)), table)
    pair = jnp.concatenate([stack_rows(geo[1]), stack_rows(geo[2])], axis=1) * gradient
    rest = unstack_rows(matmul(halves(pair), table, transposed=True))
    first = first_direction(tables, 32, first)
    masses = tiles_of(mass[...].astype(jnp.float32))
    local = [a + b + m * u for a, b, m, u in zip(first, rest, masses, tiles)]
    blocks = local_assemble(blocks_of(local, dims))
    applied_out[...] = join(blocks)
    diag_blocks = split(diag, dims)
    dev_low[...] = pack_dev([blocks, diag_blocks], 0, 0)
    dev_high[...] = pack_dev([blocks, diag_blocks], dims[0] - 1, NP - 1)
    group_low[...] = pack_group([blocks, diag_blocks], False)
    group_high[...] = pack_group([blocks, diag_blocks], True)


def products_kernel(
    dims,
    field,
    diag,
    dev_before,
    dev_after,
    group_before,
    group_after,
    residual,
    smooth,
    applied_out,
    inverse_out,
    sums_out,
):
    full = []
    for index, ref in enumerate((field, diag)):
        blocks = add_dev(split(ref, dims), index, dev_before[...], dev_after[...])
        blocks = add_group(blocks, index, group_before, group_after)
        full.append([jnp.concatenate(tile, axis=0) for tile in blocks])
    sums = [None] * 4
    for t in range(TILES):
        window = slice(t * LANES, (t + 1) * LANES)
        weight = lane_weights(t)
        applied = full[0][t]
        inverse = 1.0 / full[1][t]
        applied_out[:, window] = applied
        inverse_out[:, window] = inverse
        res = residual[:, window]
        weighted = weight * inverse
        terms = (
            weighted * res * res,
            weight * smooth[:, window] * applied,
            weighted * res * applied,
            weighted * applied * applied,
        )
        sums = [term if s is None else s + term for s, term in zip(sums, terms)]
    lane = lanes(1)
    row = jnp.zeros((1, LANES), jnp.float32)
    for n, total in enumerate(sums):
        column = jnp.sum(total, axis=0, keepdims=True)
        row = jnp.where(lane == n, jnp.sum(column, axis=1, keepdims=True), row)
    sums_out[...] = jnp.broadcast_to(row.reshape(1, 1, LANES), sums_out.shape)


def middle_kernel(parts, sums_out):
    total = jnp.sum(parts[...], axis=0, keepdims=True)
    sums_out[...] = jnp.broadcast_to(total, sums_out.shape)


def final_kernel(
    parts, solution, residual, smooth, applied, inverse, solution_out, residual_out, direction_out
):
    total = jnp.sum(parts[...], axis=0)
    norm_now, curvature, cross, quad = (total[:, n : n + 1] for n in range(4))
    step = norm_now / curvature
    norm_next = norm_now - 2.0 * step * cross + step * step * quad
    ratio = norm_next / norm_now
    direction = smooth[...]
    res = residual[...] - step * applied[...]
    solution_out[...] = solution[...] + step * direction
    residual_out[...] = res
    direction_out[...] = res * inverse[...] + ratio * direction


def call(kernel, shapes, *args):
    typed = [s if isinstance(s[1], type) else (s, jnp.float32) for s in shapes]
    outs = tuple(jax.ShapeDtypeStruct(shape, dtype) for shape, dtype in typed)
    vmem = pl.BlockSpec(memory_space=pltpu.VMEM)
    return pl.pallas_call(
        kernel,
        out_shape=outs,
        in_specs=[vmem] * len(args),
        out_specs=(vmem,) * len(outs),
        compiler_params=pltpu.CompilerParams(vmem_limit_bytes=8 * 2**20),
    )(*args)


def both_ways(low, high, axis):
    peers = lax.axis_size(axis)
    up = [(i, (i + 1) % peers) for i in range(peers)]
    before = lax.ppermute(high, axis, up)
    after = lax.ppermute(low, axis, [(j, i) for i, j in up])
    return before, after


def solution(mesh):
    groups = mesh.shape["group"]
    devs = mesh.shape["dev"]

    def on_device(solution, residual, direction, geometry, mass):
        local = solution.shape
        dims = local[1:3]
        rows = dims[0] * dims[1]
        points = local[3]
        flat = (rows, points)
        face_dev = (dims[1], LANES)
        face_group = (rows, LANES)
        solution, residual, direction, mass = (
            array.reshape(flat) for array in (solution, residual, direction, mass)
        )
        geometry = geometry.reshape((3,) + flat)
        tables = jnp.asarray(lane_tables())

        def bind(kernel):
            def body(*refs):
                kernel(dims, *refs)

            body.__name__ = kernel.__name__
            return body

        def exchange(order, dev_low, dev_high, group_low, group_high):
            if order == "dev":
                dev = both_ways(dev_low, dev_high, "dev")
                faces = call(bind(corner_kernel), [face_group] * 2, group_low, group_high, *dev)
                return dev, both_ways(*faces, "group")
            group = both_ways(group_low, group_high, "group")
            faces = call(bind(corner_dev_kernel), [face_dev] * 2, dev_low, dev_high, *group)
            return both_ways(*faces, "dev"), group

        field, dev_low, dev_high, group_low, group_high = call(
            bind(start_kernel),
            [flat, face_dev, face_dev, face_group, face_group],
            direction,
        )
        diag, tables, *plane = call(
            bind(diagonal_kernel),
            [flat, tables.shape] + [((LANES, 2 * LANES), jnp.bfloat16)] * 2,
            geometry,
            mass,
            tables,
        )
        dev, group = exchange(ORDERS[0], dev_low, dev_high, group_low, group_high)
        smooth, applied, dev_low, dev_high, group_low, group_high = call(
            bind(operator_kernel),
            [flat, flat, face_dev, face_dev, face_group, face_group],
            field,
            *dev,
            *group,
            geometry,
            mass,
            tables,
            *plane,
            diag,
        )
        dev, group = exchange(ORDERS[1], dev_low, dev_high, group_low, group_high)
        applied, inverse, sums = call(
            bind(products_kernel),
            [flat, flat, (groups, 1, LANES)],
            applied,
            diag,
            *dev,
            *group,
            residual,
            smooth,
        )
        sums = lax.all_to_all(sums, "group", 0, 0)
        (sums,) = call(middle_kernel, [(devs, 1, LANES)], sums)
        sums = lax.all_to_all(sums, "dev", 0, 0)
        outs = call(
            final_kernel, [flat] * 3, sums, solution, residual, smooth, applied, inverse
        )
        return tuple(out.reshape(local) for out in outs)

    spec = P("group", "dev", None, None)
    return jax.shard_map(
        on_device,
        mesh=mesh,
        in_specs=(spec, spec, spec, P(None, "group", "dev", None, None), spec),
        out_specs=(spec, spec, spec),
        check_vma=False,
    )
```
